256 devices in a mesh: nest: 4 (over y), tile: 64 (over z, x, core).
Axes of the slice: x: 4, y: 4, z: 8, core: 2. Of those that a mesh axis runs over, the one named last changes fastest.
Arguments:
- child_fields: float32 [4, 32, 1536, 3072], P('nest', None, 'tile'), may hold values from -18 to 18
- row_weights: float32 [8, 24], replicated
- col_weights: float32 [3072, 1024], replicated
- nest_offsets: int32 [4, 2], replicated, may hold values from 0 to 1023, as said below
- priority: int32 [1024, 1024], P('tile', 'nest'), may hold values from -1 to 3, as said below
- parent_old: float32 [32, 1024, 1024], P(None, 'tile', 'nest'), may hold values from -6 to 6
- smooth_rate: float32 [32], replicated, may hold values from 0.03 to 0.22
Outputs:
- parent_new: float32 [32, 1024, 1024], P(None, 'tile', 'nest')
The draws below stay inside these ranges and needn't reach their ends.
Inputs may be any that keep to these rules, and one draw needn't show every extreme that they name: nest_offsets[n, 0] lies in 0 .. 512 and nest_offsets[n, 1] in 0 .. 1023. priority[x, y] is -1 or a nest n with nest_offsets[n, 0] <= y < nest_offsets[n, 0] + 512.
All inputs are finite; a program needn't handle non-finite values.
Results may differ from the reference program's by a relative error of at most 0.000058.
Values sent between devices are 32-bit elements; how exact they have to be, the bound alone decides.
A program may use at most 128 MiB of HBM per device.

```python
import math
import jax
import jax.numpy as jnp
from jax import lax

CROW = 24
FL = 32
PRD = 8
PCOLS = 1024
CW = 3072
CROWS_ALL = 1536
NR = 512
PROWS_ALL = 1024
NESTS = 4


def nest_layout(key):
    key_top, key_left, key_score, key_skip, key_order = jax.random.split(jax.random.fold_in(key, 7), 5)
    top_rows = jax.random.randint(key_top, (NESTS,), 0, PROWS_ALL - NR + 1)
    left_cols = jax.random.randint(key_left, (NESTS,), 0, PCOLS)
    order = jax.random.permutation(key_order, NESTS)
    top_rows = top_rows.at[order[0]].set(PROWS_ALL - NR)
    top_rows = top_rows.at[order[1 % NESTS]].set(0)
    left_cols = left_cols.at[order[2 % NESTS]].set(PCOLS - 1)
    left_cols = left_cols.at[order[3 % NESTS]].set(0)
    row_ids = jnp.arange(PROWS_ALL)
    covered = (row_ids[None, :] >= top_rows[:, None]) & (row_ids[None, :] < top_rows[:, None] + NR)
    scores = jax.random.randint(key_score, (NESTS, PCOLS, PROWS_ALL), 0, 1000) * NESTS + jnp.arange(NESTS)[:, None, None]
    scores = jnp.where(covered[:, None, :], scores, -1)
    chosen = jnp.argmax(scores, axis=0).astype(jnp.int32)
    any_cover = jnp.any(covered, axis=0)
    skipped = jax.random.randint(key_skip, (PCOLS, PROWS_ALL), 0, 4) == 0
    priority_map = jnp.where(any_cover[None, :] & jnp.logical_not(skipped), chosen, -1)
    offsets = jnp.stack([top_rows, left_cols], axis=1)
    return (offsets.astype(jnp.int32), priority_map.astype(jnp.int32))


def draw_nest_offsets(key, part):
    return nest_layout(key)[0]


def draw_priority(key, part):
    return nest_layout(key)[1]


def draw_row_weights(key, part):
    tap_weights = jax.random.uniform(key, (PRD, 3), jnp.float32, 0.5, 1.5)
    tap_weights = tap_weights / jnp.sum(tap_weights, axis=1, keepdims=True)
    col_ids = jnp.arange(CROW)
    parent_ids = jnp.arange(PRD)
    matrix = jnp.zeros((PRD, CROW), jnp.float32)
    for member in range(3):
        matrix = matrix + tap_weights[:, member:member + 1] * (col_ids[None, :] == 3 * parent_ids[:, None] + member).astype(jnp.float32)
    return matrix


def draw_col_weights(key, part):
    key_inner, key_outer = jax.random.split(key)
    inner = jax.random.uniform(key_inner, (PCOLS, 3), jnp.float32, 0.5, 1.5)
    outer = jax.random.uniform(key_outer, (PCOLS, 2), jnp.float32, 0.1, 0.5)
    tap_weights = jnp.concatenate([outer[:, :1], inner, outer[:, 1:]], axis=1)
    tap_weights = tap_weights / jnp.sum(tap_weights, axis=1, keepdims=True)
    child_ids = jnp.arange(CW)
    parent_ids = jnp.arange(PCOLS)
    matrix = jnp.zeros((CW, PCOLS), jnp.float32)
    for member in range(5):
        target = (3 * parent_ids + member - 1) % CW
        matrix = matrix + tap_weights[None, :, member] * (child_ids[:, None] == target[None, :]).astype(jnp.float32)
    return matrix


def block_levels(key, extent, pieces, smallest, largest):
    loudness, own = 1.0, jax.random.fold_in(key, 6)
    for dim, shards_of in pieces:
        heights = jnp.exp(jax.random.uniform(jax.random.fold_in(own, dim), (shards_of,), jnp.float32, smallest / len(pieces), largest / len(pieces)))
        loudness = loudness * jnp.repeat(heights, extent[dim] // shards_of).reshape([-1 if axis == dim else 1 for axis in range(len(extent))])
    return loudness


def normal_values(key, dims, deviation, limit, cuts=(), kind=jnp.bfloat16):
    gain = block_levels(key, dims, cuts, -0.22, 0.18) if cuts else 1.0
    entries = jax.random.normal(key, dims, jnp.float32) * deviation * gain
    return jnp.minimum(jnp.maximum(entries, -limit), limit).astype(kind)


def setup_inputs(seed: int = 0) -> dict:
    key_list = jax.random.split(jax.random.key(seed), 8)
    child_fields = normal_values(key_list[0], (NESTS, FL, CROWS_ALL, CW), 3.0, 18.0, ((0, 4), (2, 64)), jnp.float32)
    row_weights = draw_row_weights(jax.random.fold_in(key_list[7], 71), 0)
    col_weights = draw_col_weights(jax.random.fold_in(key_list[7], 71), 0)
    nest_offsets = draw_nest_offsets(jax.random.fold_in(key_list[7], 71), 0)
    priority = draw_priority(jax.random.fold_in(key_list[7], 71), 0)
    parent_old = normal_values(key_list[5], (FL, PCOLS, PROWS_ALL), 1.0, 6.0, ((1, 64), (2, 4)), jnp.float32)
    smooth_rate = jnp.clip(jnp.exp(jax.random.uniform(key_list[6], (FL,), jnp.float32, math.log(0.03), math.log(0.22))), 0.03, 0.22)
    return {"child_fields": child_fields, "row_weights": row_weights, "col_weights": col_weights, "nest_offsets": nest_offsets, "priority": priority, "parent_old": parent_old, "smooth_rate": smooth_rate}


def reference(child_fields, row_weights, col_weights, nest_offsets, priority, parent_old, smooth_rate):
    nest_count, planes, crows_all, child_cols = child_fields.shape
    cell_rows, child_rows = row_weights.shape
    row_blocks = crows_all // child_rows
    nrows = row_blocks * cell_rows

    def restrict_one(child_block):
        grouped = child_block.reshape(planes, row_blocks, child_rows, child_cols)
        thinned = jnp.einsum('pr,ftrc->ftpc', row_weights, grouped, precision=lax.Precision.HIGHEST)
        thinned = thinned.reshape(planes, nrows, child_cols)
        return jnp.einsum('fyc,cx->fxy', thinned, col_weights, precision=lax.Precision.HIGHEST)

    restricted = lax.map(restrict_one, child_fields)
    merged = parent_old
    for nest_num in range(nest_count):
        rolled = jnp.roll(restricted[nest_num], nest_offsets[nest_num, 1], axis=1)
        placed = lax.dynamic_update_slice(jnp.zeros_like(parent_old), rolled,
                                          (jnp.int32(0), jnp.int32(0), nest_offsets[nest_num, 0].astype(jnp.int32)))
        merged = jnp.where((priority == nest_num)[None], placed, merged)
    east_side = jnp.roll(merged, -1, axis=1)
    west_side = jnp.roll(merged, 1, axis=1)
    padded = jnp.concatenate([merged[:, :, :1], merged, merged[:, :, -1:]], axis=2)
    north_side = padded[:, :, 2:]
    south_side = padded[:, :, :-2]
    return merged + smooth_rate[:, None, None] * (east_side + west_side + north_side + south_side - 4.0 * merged)
```

```python
import jax
import jax.numpy as jnp
from jax import lax
from jax.experimental import pallas as pl
from jax.experimental.pallas import tpu as pltpu
from jax.sharding import PartitionSpec as P

MESH = pl.DeviceIdType.MESH
CELL = 8
FC = 16
XB = 16
LANES = XB * FC
TILED = LANES // 128


def swap_rows_and_groups(v):
    sub = lax.broadcasted_iota(jnp.int32, v.shape, 0)
    lane = lax.broadcasted_iota(jnp.int32, v.shape, 1)
    for d in (1, 2, 4):
        w = FC * d
        low = pltpu.roll(pltpu.roll(v, CELL - d, 0), w, 1)
        high = pltpu.roll(pltpu.roll(v, d, 0), 128 - w, 1)
        sbit, lbit = (sub & d) != 0, (lane & w) != 0
        v = jnp.where(sbit == lbit, v, jnp.where(lbit, low, high))
    return v


def exchange_kernel(
    offs, rate, g_ref, prio_ref, par_ref, out_ref,
    gt, snd, slab, half, q, mrg, nat, part, prit, edge, halo, fin, parv, outv,
    ps, os, zs, zr, ys, yr, hs, hr,
):
    n, me = lax.axis_index("nest"), lax.axis_index("tile")
    tiles, nests = lax.axis_size("tile"), lax.axis_size("nest")
    cols, rows = tiles * XB, tiles * CELL
    own = par_ref.shape[1]
    chunks = snd.shape[0]
    top, left = offs[n, 0], offs[n, 1]

    span = min(128, own)
    taken = [
        pltpu.make_async_copy(par_ref.at[:, pl.ds(b * span, span)], parv.at[b], ps.at[b]) for b in range(own // span)
    ]
    for c in taken:
        c.start()

    barrier = pltpu.get_barrier_semaphore()

    @pl.loop(1, tiles)
    def _(j):
        pl.semaphore_signal(barrier, inc=1, device_id=(n, lax.rem(me + j, tiles)), device_id_type=MESH)

    for dn in range(1, nests):
        pl.semaphore_signal(barrier, inc=1, device_id=(lax.rem(n + dn, nests), me), device_id_type=MESH)

    def prepare(k):
        wide = min(128, cols)
        for b in range(cols // wide):
            gt[k, b * wide : (b + 1) * wide, :] = g_ref[k * 128 : (k + 1) * 128, b * wide : (b + 1) * wide].T
        gt[k, cols : cols + 8, :] = gt[k, 0:8, :]

        @pl.loop(0, tiles, step=4)
        def _(j0):
            for dj in range(4):
                for h in range(2):
                    s = lax.rem(XB * (j0 + dj) + 8 * h - left + cols, cols)
                    snd[k, j0 + dj, h] = swap_rows_and_groups(gt[k, pl.ds(s, 8), :])

    def send_tiles(k):
        @pl.loop(0, tiles - 1)
        def _(i):
            j = lax.select(lax.rem(i, 2) == 0, i // 2 + 1, tiles - 1 - i // 2)
            d = lax.rem(me + j, tiles)
            pltpu.make_async_remote_copy(
                src_ref=snd.at[k, d],
                dst_ref=slab[k].at[:, pl.ds(pl.multiple_of(CELL * me, CELL), CELL), :],
                send_sem=zs.at[k],
                recv_sem=zr.at[k],
                device_id=(n, d),
                device_id_type=MESH,
            ).start()

        slab[k][:, pl.ds(pl.multiple_of(CELL * me, CELL), CELL), :] = snd[k, me]

    def send_nests(k):
        got = slab[k].at[:, pl.ds(0, rows - CELL), :]
        pltpu.make_async_copy(got, got, zr.at[k]).wait()
        slab[k][:, rows : rows + 8, :] = slab[k][:, 0:8, :]

        @pl.loop(0, rows // 8)
        def _(g):
            s = lax.rem(8 * g - top + rows, rows)
            for t in range(TILED):
                half[k, t, pl.ds(pl.multiple_of(8 * g, 8), 8), :] = slab[k][t, pl.ds(s, 8), :]

        for dn in range(1, nests):
            b = lax.rem(n + dn, nests)
            start = pl.multiple_of(lax.rem(b * own, rows), own)
            pltpu.make_async_remote_copy(
                src_ref=half.at[k, :, pl.ds(start, own), :],
                dst_ref=q.at[k, n],
                send_sem=ys.at[k],
                recv_sem=yr.at[k],
                device_id=(b, me),
                device_id_type=MESH,
            ).start()
        mine = pl.multiple_of(lax.rem(n * own, rows), own)

        @pl.loop(0, own // 8)
        def _(g):
            r = pl.multiple_of(8 * g, 8)
            q[k, n, :, pl.ds(r, 8), :] = half[k, :, pl.ds(mine + r, 8), :]

    def to_rows(dst):
        for lb in range(TILED):
            for yb in range(own // span):
                dst[lb, yb * span : (yb + 1) * span, :] = nat[
                    lb * 128 : (lb + 1) * 128, yb * span : (yb + 1) * span
                ].T

    def own_rows():
        for x in range(XB):
            nat[x * FC : (x + 1) * FC, :] = jnp.broadcast_to(prio_ref[x : x + 1, :].astype(jnp.float32), (FC, own))
        to_rows(prit)
        for c in taken:
            c.wait()
        for k in range(chunks):
            for x in range(XB):
                for b in range(own // span):
                    nat[x * FC : (x + 1) * FC, b * span : (b + 1) * span] = parv[b, pl.ds(k * LANES + x, FC, stride=XB), :]
            to_rows(part.at[k])

    packs = min(8, own // 8)
    packed = own // packs
    lane = lax.broadcasted_iota(jnp.int32, (8, 128), 1)

    def merge(k):
        got = q.at[k, pl.ds(0, nests - 1)]
        pltpu.make_async_copy(got, got, yr.at[k]).wait()

        @pl.loop(0, own // 8)
        def _(g):
            r = pl.ds(pl.multiple_of(8 * g, 8), 8)
            v, p = part[k, :, r, :], prit[:, r, :]
            for m in range(nests):
                v = jnp.where(p == float(m), q[k, m, :, r, :], v)
            mrg[k, :, pl.ds(pl.multiple_of(8 * g + 8, 8), 8), :] = v

        for i in range(packed // 8):
            first = last = jnp.zeros((8, 128), jnp.float32)
            for j in range(packs):
                r = 8 + packed * j + 8 * i
                a, b = mrg[k, 0, r : r + 8, :], mrg[k, TILED - 1, r : r + 8, :]
                here = lane // FC == j
                first = jnp.where(here, pltpu.roll(a, FC * j, 1) if j else a, first)
                shift = (FC * j + FC) % 128
                last = jnp.where(here, pltpu.roll(b, shift, 1) if shift else b, last)
            edge[k, 0, 8 * i : 8 * i + 8, :] = first
            edge[k, 1, 8 * i : 8 * i + 8, :] = last

        east, west = lax.rem(me + 1, tiles), lax.rem(me + tiles - 1, tiles)
        up, down = lax.rem(n + 1, nests), lax.rem(n + nests - 1, nests)
        moves = (
            (edge.at[k, 0], halo.at[k, 0], (n, west)),
            (edge.at[k, 1], halo.at[k, 1], (n, east)),
            (mrg.at[k, :, pl.ds(8, 8), :], mrg.at[k, :, pl.ds(own + 8, 8), :], (down, me)),
            (mrg.at[k, :, pl.ds(own, 8), :], mrg.at[k, :, pl.ds(0, 8), :], (up, me)),
        )
        copies = [
            pltpu.make_async_remote_copy(
                src_ref=s, dst_ref=d, send_sem=hs.at[k, i], recv_sem=hr.at[k, i], device_id=to, device_id_type=MESH
            )
            for i, (s, d, to) in enumerate(moves)
        ]
        for c in copies:
            c.start()
        return copies

    def finish(k, copies):
        for c in copies:
            c.wait()
        mrg[k, :, 7:8, :] = jnp.where(n == 0, mrg[k, :, 8:9, :], mrg[k, :, 7:8, :])
        mrg[k, :, own + 8 : own + 9, :] = jnp.where(
            n == nests - 1, mrg[k, :, own + 7 : own + 8, :], mrg[k, :, own + 8 : own + 9, :]
        )
        r = jnp.zeros((8, 128), jnp.float32)
        for f in range(FC):
            r = jnp.where(lax.rem(lane, FC) == f, rate[k * FC + f], r)

        for j in range(packs):
            @pl.loop(0, packed // 8)
            def _(i):
                o = pl.multiple_of(packed * j + 8 * i, 8)
                e = halo[k, 0, pl.ds(pl.multiple_of(8 * i, 8), 8), :]
                w = halo[k, 1, pl.ds(pl.multiple_of(8 * i, 8), 8), :]
                es, ws = (128 - FC - FC * j) % 128, (128 - FC * j) % 128
                e = pltpu.roll(e, es, 1) if es else e
                w = pltpu.roll(w, ws, 1) if ws else w
                mid = [mrg[k, t, pl.ds(o + 8, 8), :] for t in range(TILED)]
                east = [pltpu.roll(c, 128 - FC, 1) for c in mid] + [e]
                west = [w] + [pltpu.roll(c, FC, 1) for c in mid]
                for t in range(TILED):
                    c = mid[t]
                    north, south = mrg[k, t, pl.ds(o + 9, 8), :], mrg[k, t, pl.ds(o + 7, 8), :]
                    east_side = jnp.where(lane >= 128 - FC, east[t + 1], east[t])
                    west_side = jnp.where(lane < FC, west[t], west[t + 1])
                    fin[t, pl.ds(o, 8), :] = c + r * (east_side + west_side + north + south - 4.0 * c)

        for lb in range(TILED):
            for yb in range(own // span):
                t = fin[lb, yb * span : (yb + 1) * span, :].T
                for x in range(8):
                    outv[yb, pl.ds(k * LANES + lb * 8 + x, FC, stride=XB), :] = t[x * FC : (x + 1) * FC, :]
        r = pl.ds(k * LANES, LANES)
        for b in range(own // span):
            c = pltpu.make_async_copy(outv.at[b, r, :], out_ref.at[r, pl.ds(b * span, span)], os.at[k, b])
            c.start()
            given.append(c)

    prepare(0)
    pl.semaphore_wait(barrier, tiles - 1 + nests - 1)
    send_tiles(0)
    for k in range(1, chunks):
        prepare(k)
        send_tiles(k)
    own_rows()
    flights, given = [], []
    for k in range(chunks):
        send_nests(k)
        if k:
            flights.append(merge(k - 1))
            if k > 1:
                finish(k - 2, flights[k - 2])
    flights.append(merge(chunks - 1))
    if chunks > 1:
        finish(chunks - 2, flights[chunks - 2])
    finish(chunks - 1, flights[chunks - 1])
    for c in given:
        c.wait()
    for k in range(chunks):
        sent = slab[k].at[:, pl.ds(0, rows - CELL), :]
        pltpu.make_async_copy(sent, sent, zs.at[k]).wait()
        sent = q.at[k, pl.ds(0, nests - 1)]
        pltpu.make_async_copy(sent, sent, ys.at[k]).wait()


def exchange(offs, rate, g, prio, par, tiles, nests):
    own = par.shape[1]
    fields = par.shape[0] // XB
    chunks = fields // FC
    cols, rows = tiles * XB, tiles * CELL
    span = min(128, own)
    f32 = jnp.float32
    vm = pl.BlockSpec(memory_space=pltpu.VMEM)
    sm = pl.BlockSpec(memory_space=pltpu.SMEM)
    dma = pltpu.SemaphoreType.DMA
    return pl.pallas_call(
        exchange_kernel,
        out_shape=jax.ShapeDtypeStruct(par.shape, f32),
        in_specs=[sm, sm, vm, vm, pl.BlockSpec(memory_space=pl.ANY)],
        out_specs=pl.BlockSpec(memory_space=pl.ANY),
        scratch_shapes=[
            pltpu.VMEM((chunks, cols + 8, 128), f32),
            pltpu.VMEM((chunks, tiles, TILED, CELL, 128), f32),
            [pltpu.VMEM((TILED, rows + 8, 128), f32) for _ in range(chunks)],
            pltpu.VMEM((chunks, TILED, rows, 128), f32),
            pltpu.VMEM((chunks, nests, TILED, own, 128), f32),
            pltpu.VMEM((chunks, TILED, own + 16, 128), f32),
            pltpu.VMEM((LANES, own), f32),
            pltpu.VMEM((chunks, TILED, own, 128), f32),
            pltpu.VMEM((TILED, own, 128), f32),
            pltpu.VMEM((chunks, 2, own // min(8, own // 8), 128), f32),
            pltpu.VMEM((chunks, 2, own // min(8, own // 8), 128), f32),
            pltpu.VMEM((TILED, own, 128), f32),
            pltpu.VMEM((own // span, *par.shape[:1], span), f32),
            pltpu.VMEM((own // span, *par.shape[:1], span), f32),
            dma((own // span,)), dma((chunks, own // span)),
            dma((chunks,)), dma((chunks,)), dma((chunks,)), dma((chunks,)), dma((chunks, 4)), dma((chunks, 4)),
        ],
        compiler_params=pltpu.CompilerParams(
            collective_id=0, has_side_effects=True, vmem_limit_bytes=40 * 1024 * 1024
        ),
    )(offs, rate, g, prio, par)


def per_device(child_fields, row_weights, col_weights, nest_offsets, priority, parent_old, smooth_rate):
    fields, strip, own = parent_old.shape
    tiles, nests = lax.axis_size("tile"), lax.axis_size("nest")
    child = child_fields[0].reshape(fields // FC, FC, *child_fields.shape[2:])
    high = lax.Precision.HIGH
    thinned = jnp.einsum("pr,kfrc->kpfc", row_weights, child, precision=high)
    thinned = thinned.reshape(fields * CELL, -1)
    g = jnp.einsum("mc,cx->mx", thinned, col_weights, precision=high)
    out = exchange(nest_offsets, smooth_rate, g, priority, parent_old.reshape(fields * strip, own), tiles, nests)
    return out.reshape(fields, strip, own)


def solution(mesh):
    return jax.shard_map(
        per_device,
        mesh=mesh,
        in_specs=(
            P("nest", None, "tile", None),
            P(),
            P(),
            P(),
            P("tile", "nest"),
            P(None, "tile", "nest"),
            P(),
        ),
        out_specs=P(None, "tile", "nest"),
        check_vma=False,
    )
```

```python
import jax
import jax.numpy as jnp
from jax import lax
from jax.experimental import pallas as pl
from jax.experimental.pallas import tpu as pltpu
from jax.sharding import PartitionSpec as P

MESH = pl.DeviceIdType.MESH
CELL = 8
FC = 16
XB = 16
TILED = XB * FC // 128
AHEAD = 3
f32, bf16 = jnp.float32, jnp.bfloat16


def swap_rows_and_groups(v):
    sub = lax.broadcasted_iota(jnp.int32, v.shape, 0)
    lane = lax.broadcasted_iota(jnp.int32, v.shape, 1)
    for d in (1, 2, 4):
        w = FC * d
        low = pltpu.roll(pltpu.roll(v, CELL - d, 0), w, 1)
        high = pltpu.roll(pltpu.roll(v, d, 0), 128 - w, 1)
        sbit, lbit = (sub & d) != 0, (lane & w) != 0
        v = jnp.where(sbit == lbit, v, jnp.where(lbit, low, high))
    return v


def two_parts(v):
    high = v.astype(bf16)
    return high, (v - high.astype(f32)).astype(bf16)


def mm(a, b):
    return jnp.dot(a, b, preferred_element_type=f32)


def kernel(
    offs, rate, child, row_w, col_w, prio_ref, par_ref, out_ref,
    xbuf, cbuf, whi, wlo, wide_w, acc,
    gt, snd, slab, half, q, mrg, nat, part, prit, edge, halo, fin, parv, outv,
    cs, ws, ps, os, zs, zr, ys, yr, hs, hr,
):
    n, me = lax.axis_index("nest"), lax.axis_index("tile")
    tiles, nests = lax.axis_size("tile"), lax.axis_size("nest")
    cols, rows = tiles * XB, tiles * CELL
    own = par_ref.shape[1]
    chunks, pieces, depth, piece = xbuf.shape
    crow = row_w.shape[1]
    top, left = offs[n, 0], offs[n, 1]
    high = FC * CELL

    def child_copy(k, c):
        start = c * piece if isinstance(c, int) else pl.multiple_of(c * piece, 128)
        return pltpu.make_async_copy(
            child.at[pl.ds(k * depth, depth), pl.ds(start, piece)], xbuf.at[k, c], cs.at[k, c]
        )

    def weight_copy(c):
        start = c * piece if isinstance(c, int) else pl.multiple_of(c * piece, 128)
        return pltpu.make_async_copy(col_w.at[pl.ds(start, piece), :], cbuf.at[c], ws.at[c])

    for c in range(min(AHEAD, pieces)):
        child_copy(0, c).start()
        weight_copy(c).start()

    barrier = pltpu.get_barrier_semaphore()

    @pl.loop(1, tiles)
    def _(j):
        pl.semaphore_signal(barrier, inc=1, device_id=(n, lax.rem(me + j, tiles)), device_id_type=MESH)

    for dn in range(1, nests):
        pl.semaphore_signal(barrier, inc=1, device_id=(lax.rem(n + dn, nests), me), device_id_type=MESH)

    def spread_row_weights():
        a = lax.broadcasted_iota(jnp.int32, (high, CELL), 0)
        b = lax.broadcasted_iota(jnp.int32, (high, CELL), 1)
        down = (a // FC == b).astype(f32).astype(bf16)
        a = lax.broadcasted_iota(jnp.int32, (crow, depth), 0)
        b = lax.broadcasted_iota(jnp.int32, (crow, depth), 1)
        across = (lax.rem(b, crow) == a).astype(f32).astype(bf16)
        a = lax.broadcasted_iota(jnp.int32, (high, depth), 0)
        b = lax.broadcasted_iota(jnp.int32, (high, depth), 1)
        same = lax.rem(a, FC) == b // crow
        for i, w in enumerate(two_parts(row_w[...])):
            full = mm(mm(down, w).astype(bf16), across)
            wide_w[i * high : (i + 1) * high, :] = jnp.where(same, full, 0.0).astype(bf16)

    step = min(256, piece)
    block = min(256, cols)

    def compute(k):
        acc[k] = jnp.zeros(acc.shape[1:], f32)

        @pl.loop(0, pieces)
        def _(c):
            child_copy(k, c).wait()
            if k == 0:
                weight_copy(c).wait()

                @pl.when(c + AHEAD < pieces)
                def _():
                    child_copy(0, c + AHEAD).start()
                    weight_copy(c + AHEAD).start()

            if k + 1 < chunks:
                child_copy(k + 1, c).start()
            left_high, left_low = [], []
            for s in range(piece // step):
                xh, xl = two_parts(xbuf[k, c, :, s * step : (s + 1) * step])
                t = mm(wide_w[...], xh)
                t = t[:high] + t[high:] + mm(wide_w[0:high, :], xl)
                th, tl = two_parts(t)
                left_high.append(th)
                left_low.append(tl)
            a_high = jnp.concatenate(left_high, 1)
            a = jnp.concatenate([a_high, jnp.concatenate(left_low, 1)], 0)
            for b in range(cols // block):
                span = pl.ds(b * block, block)
                if k == 0:
                    wh, wl = two_parts(cbuf[c, :, span])
                    whi[c, :, span] = wh
                    wlo[c, :, span] = wl
                else:
                    wh, wl = whi[c, :, span], wlo[c, :, span]
                u = mm(a, wh)
                acc[k, :, span] += u[:high] + u[high:] + mm(a_high, wl)

    def turn(k):
        wide = min(128, cols)
        for b in range(cols // wide):
            gt[k, b * wide : (b + 1) * wide, :] = acc[k, :, b * wide : (b + 1) * wide].T
        gt[k, cols : cols + 8, :] = gt[k, 0:8, :]

    def send_tiles(k, h):
        @pl.loop(0, tiles, step=8)
        def _(j0):
            for dj in range(8):
                s = lax.rem(XB * (j0 + dj) + 8 * h - left + cols, cols)
                snd[k, h, j0 + dj] = swap_rows_and_groups(gt[k, pl.ds(s, 8), :])

        mine = pl.ds(pl.multiple_of(CELL * me, CELL), CELL)

        @pl.loop(0, tiles - 1)
        def _(i):
            j = lax.select(lax.rem(i, 2) == 0, i // 2 + 1, tiles - 1 - i // 2)
            d = lax.rem(me + j, tiles)
            pltpu.make_async_remote_copy(
                src_ref=snd.at[k, h, d],
                dst_ref=slab[k][h].at[mine, :],
                send_sem=zs.at[k, h],
                recv_sem=zr.at[k, h],
                device_id=(n, d),
                device_id_type=MESH,
            ).start()

        slab[k][h][mine, :] = snd[k, h, me]

    def send_nests(k, h):
        here = slab[k][h]
        got = here.at[pl.ds(0, rows - CELL), :]
        pltpu.make_async_copy(got, got, zr.at[k, h]).wait()
        here[rows : rows + 8, :] = here[0:8, :]

        @pl.loop(0, rows // 8, step=8)
        def _(g0):
            for dg in range(8):
                g = g0 + dg
                s = lax.rem(8 * g - top + rows, rows)
                half[k, h, pl.ds(pl.multiple_of(8 * g, 8), 8), :] = here[pl.ds(s, 8), :]

        for dn in (2, 1, 3):
            b = lax.rem(n + dn, nests)
            start = pl.multiple_of(lax.rem(b * own, rows), own)
            pltpu.make_async_remote_copy(
                src_ref=half.at[k, h, pl.ds(start, own), :],
                dst_ref=q.at[k, h, n],
                send_sem=ys.at[k, h],
                recv_sem=yr.at[k, h],
                device_id=(b, me),
                device_id_type=MESH,
            ).start()
        mine = pl.multiple_of(lax.rem(n * own, rows), own)

        @pl.loop(0, own // 8)
        def _(g):
            r = pl.multiple_of(8 * g, 8)
            q[k, h, n, pl.ds(r, 8), :] = half[k, h, pl.ds(mine + r, 8), :]

    span = min(128, own)
    taken = [
        pltpu.make_async_copy(par_ref.at[:, pl.ds(b * span, span)], parv.at[b], ps.at[b]) for b in range(own // span)
    ]

    def to_rows(dst):
        for lb in range(TILED):
            for yb in range(own // span):
                dst[lb, yb * span : (yb + 1) * span, :] = nat[
                    lb * 128 : (lb + 1) * 128, yb * span : (yb + 1) * span
                ].T

    def own_rows():
        for x in range(XB):
            nat[x * FC : (x + 1) * FC, :] = jnp.broadcast_to(prio_ref[x : x + 1, :].astype(f32), (FC, own))
        to_rows(prit)
        for c in taken:
            c.wait()
        for k in range(chunks):
            for x in range(XB):
                for b in range(own // span):
                    nat[x * FC : (x + 1) * FC, b * span : (b + 1) * span] = parv[
                        b, pl.ds(k * XB * FC + x, FC, stride=XB), :
                    ]
            to_rows(part.at[k])

    packs = min(8, own // 8)
    packed = own // packs
    lane = lax.broadcasted_iota(jnp.int32, (8, 128), 1)
    east, west = lax.rem(me + 1, tiles), lax.rem(me + tiles - 1, tiles)
    up, down = lax.rem(n + 1, nests), lax.rem(n + nests - 1, nests)
    flights, given = {}, []

    def merge(k, h):
        got = q.at[k, h, pl.ds(0, nests - 1)]
        pltpu.make_async_copy(got, got, yr.at[k, h]).wait()

        @pl.loop(0, own // 8, step=4)
        def _(g0):
            for dg in range(4):
                r = pl.ds(pl.multiple_of(8 * (g0 + dg), 8), 8)
                v, p = part[k, h, r, :], prit[h, r, :]
                for m in range(nests):
                    v = jnp.where(p == float(m), q[k, h, m, r, :], v)
                mrg[k, h, pl.ds(pl.multiple_of(8 * (g0 + dg) + 8, 8), 8), :] = v

        moves = [
            (mrg.at[k, h, pl.ds(8, 8), :], mrg.at[k, h, pl.ds(own + 8, 8), :], (down, me)),
            (mrg.at[k, h, pl.ds(own, 8), :], mrg.at[k, h, pl.ds(0, 8), :], (up, me)),
        ]
        for side, tile, to in ((0, 0, west), (1, TILED - 1, east)):
            if h != tile:
                continue
            for i in range(packed // 8):
                e = jnp.zeros((8, 128), f32)
                for j in range(packs):
                    a = mrg[k, h, 8 + packed * j + 8 * i : 16 + packed * j + 8 * i, :]
                    shift = (FC * (j + side)) % 128
                    e = jnp.where(lane // FC == j, pltpu.roll(a, shift, 1) if shift else a, e)
                edge[k, side, 8 * i : 8 * i + 8, :] = e
            moves.append((edge.at[k, side], halo.at[k, side], (n, to)))
        copies = [
            pltpu.make_async_remote_copy(
                src_ref=s, dst_ref=d, send_sem=hs.at[k, h, i], recv_sem=hr.at[k, h, i], device_id=to, device_id_type=MESH
            )
            for i, (s, d, to) in enumerate(moves)
        ]
        for c in copies:
            c.start()
        flights.setdefault(k, []).extend(copies)

    def finish(k):
        for c in flights[k]:
            c.wait()
        mrg[k, :, 7:8, :] = jnp.where(n == 0, mrg[k, :, 8:9, :], mrg[k, :, 7:8, :])
        mrg[k, :, own + 8 : own + 9, :] = jnp.where(
            n == nests - 1, mrg[k, :, own + 7 : own + 8, :], mrg[k, :, own + 8 : own + 9, :]
        )
        r = jnp.zeros((8, 128), f32)
        for f in range(FC):
            r = jnp.where(lax.rem(lane, FC) == f, rate[k * FC + f], r)

        for j in range(packs):
            @pl.loop(0, packed // 8)
            def _(i):
                o = pl.multiple_of(packed * j + 8 * i, 8)
                e = halo[k, 0, pl.ds(pl.multiple_of(8 * i, 8), 8), :]
                w = halo[k, 1, pl.ds(pl.multiple_of(8 * i, 8), 8), :]
                es, ws_ = (128 - FC - FC * j) % 128, (128 - FC * j) % 128
                e = pltpu.roll(e, es, 1) if es else e
                w = pltpu.roll(w, ws_, 1) if ws_ else w
                mid = [mrg[k, t, pl.ds(o + 8, 8), :] for t in range(TILED)]
                east_of = [pltpu.roll(c, 128 - FC, 1) for c in mid] + [e]
                west_of = [w] + [pltpu.roll(c, FC, 1) for c in mid]
                for t in range(TILED):
                    c = mid[t]
                    north, south = mrg[k, t, pl.ds(o + 9, 8), :], mrg[k, t, pl.ds(o + 7, 8), :]
                    east_side = jnp.where(lane >= 128 - FC, east_of[t + 1], east_of[t])
                    west_side = jnp.where(lane < FC, west_of[t], west_of[t + 1])
                    fin[t, pl.ds(o, 8), :] = c + r * (east_side + west_side + north + south - 4.0 * c)

        for lb in range(TILED):
            for yb in range(own // span):
                t = fin[lb, yb * span : (yb + 1) * span, :].T
                for x in range(8):
                    outv[yb, pl.ds(k * XB * FC + lb * 8 + x, FC, stride=XB), :] = t[x * FC : (x + 1) * FC, :]
        r = pl.ds(k * XB * FC, XB * FC)
        for b in range(own // span):
            c = pltpu.make_async_copy(outv.at[b, r, :], out_ref.at[r, pl.ds(b * span, span)], os.at[k, b])
            c.start()
            given.append(c)

    spread_row_weights()
    for k in range(chunks):
        compute(k)
        if k == 0:
            for c in taken:
                c.start()
            pl.semaphore_wait(barrier, tiles - 1 + nests - 1)
        turn(k)
        for h in range(TILED):
            send_tiles(k, h)
    own_rows()
    order = [(k, h) for k in range(chunks) for h in range(TILED)]
    for i, (k, h) in enumerate(order):
        send_nests(k, h)
        if i >= 2:
            merge(*order[i - 2])
            if order[i - 2][1] == TILED - 1 and i < len(order) - 1:
                finish(order[i - 2][0])
    for k, h in order[-2:]:
        if h == 0 and k > 0:
            finish(k - 1)
        merge(k, h)
    finish(chunks - 1)
    for c in given:
        c.wait()
    for k, h in order:
        sent = slab[k][h].at[pl.ds(0, rows - CELL), :]
        pltpu.make_async_copy(sent, sent, zs.at[k, h]).wait()
        sent = q.at[k, h, pl.ds(0, nests - 1)]
        pltpu.make_async_copy(sent, sent, ys.at[k, h]).wait()


def feedback(offs, rate, child, row_w, col_w, prio, par, tiles, nests):
    own = par.shape[1]
    chunks = par.shape[0] // XB // FC
    cols, rows = tiles * XB, tiles * CELL
    span = min(128, own)
    depth = FC * row_w.shape[1]
    width = child.shape[1]
    pieces = min(6, width // 128)
    piece = width // pieces
    packed = own // min(8, own // 8)
    vm = pl.BlockSpec(memory_space=pltpu.VMEM)
    sm = pl.BlockSpec(memory_space=pltpu.SMEM)
    hbm = pl.BlockSpec(memory_space=pl.ANY)
    dma = pltpu.SemaphoreType.DMA
    return pl.pallas_call(
        kernel,
        out_shape=jax.ShapeDtypeStruct(par.shape, f32),
        in_specs=[sm, sm, hbm, vm, hbm, vm, hbm],
        out_specs=hbm,
        scratch_shapes=[
            pltpu.VMEM((chunks, pieces, depth, piece), f32),
            pltpu.VMEM((pieces, piece, cols), f32),
            pltpu.VMEM((pieces, piece, cols), bf16),
            pltpu.VMEM((pieces, piece, cols), bf16),
            pltpu.VMEM((2 * FC * CELL, depth), bf16),
            pltpu.VMEM((chunks, FC * CELL, cols), f32),
            pltpu.VMEM((chunks, cols + 8, 128), f32),
            pltpu.VMEM((chunks, TILED, tiles, CELL, 128), f32),
            [[pltpu.VMEM((rows + 8, 128), f32) for _ in range(TILED)] for _ in range(chunks)],
            pltpu.VMEM((chunks, TILED, rows, 128), f32),
            pltpu.VMEM((chunks, TILED, nests, own, 128), f32),
            pltpu.VMEM((chunks, TILED, own + 16, 128), f32),
            pltpu.VMEM((XB * FC, own), f32),
            pltpu.VMEM((chunks, TILED, own, 128), f32),
            pltpu.VMEM((TILED, own, 128), f32),
            pltpu.VMEM((chunks, 2, packed, 128), f32),
            pltpu.VMEM((chunks, 2, packed, 128), f32),
            pltpu.VMEM((TILED, own, 128), f32),
            pltpu.VMEM((own // span, par.shape[0], span), f32),
            pltpu.VMEM((own // span, par.shape[0], span), f32),
            dma((chunks, pieces)), dma((pieces,)), dma((own // span,)), dma((chunks, own // span)),
            dma((chunks, TILED)), dma((chunks, TILED)), dma((chunks, TILED)), dma((chunks, TILED)),
            dma((chunks, TILED, 4)), dma((chunks, TILED, 4)),
        ],
        compiler_params=pltpu.CompilerParams(
            collective_id=0, has_side_effects=True, vmem_limit_bytes=60 * 1024 * 1024
        ),
    )(offs, rate, child, row_w, col_w, prio, par)


def per_device(child_fields, row_weights, col_weights, nest_offsets, priority, parent_old, smooth_rate):
    fields, strip, own = parent_old.shape
    tiles, nests = lax.axis_size("tile"), lax.axis_size("nest")
    child = child_fields.reshape(-1, child_fields.shape[3])
    par = parent_old.reshape(fields * strip, own)
    out = feedback(nest_offsets, smooth_rate, child, row_weights, col_weights, priority, par, tiles, nests)
    return out.reshape(fields, strip, own)


def solution(mesh):
    return jax.shard_map(
        per_device,
        mesh=mesh,
        in_specs=(
            P("nest", None, "tile", None),
            P(),
            P(),
            P(),
            P("tile", "nest"),
            P(None, "tile", "nest"),
            P(),
        ),
        out_specs=P(None, "tile", "nest"),
        check_vma=False,
    )
```

```python
import jax
import jax.numpy as jnp
from jax import lax
from jax.experimental import pallas as pl
from jax.experimental.pallas import tpu as pltpu
from jax.sharding import PartitionSpec as P

MESH = pl.DeviceIdType.MESH
CELL = 8
FC = 16
XB = 16
TILED = XB * FC // 128
AHEAD = 3
f32, bf16 = jnp.float32, jnp.bfloat16


def swap_rows_and_groups(v):
    sub = lax.broadcasted_iota(jnp.int32, v.shape, 0)
    lane = lax.broadcasted_iota(jnp.int32, v.shape, 1)
    for d in (1, 2, 4):
        w = FC * d
        low = pltpu.roll(pltpu.roll(v, CELL - d, 0), w, 1)
        high = pltpu.roll(pltpu.roll(v, d, 0), 128 - w, 1)
        sbit, lbit = (sub & d) != 0, (lane & w) != 0
        v = jnp.where(sbit == lbit, v, jnp.where(lbit, low, high))
    return v


def two_parts(v):
    high = v.astype(bf16)
    return high, (v - high.astype(f32)).astype(bf16)


def mm(a, b):
    return jnp.dot(a, b, preferred_element_type=f32)


def kernel(
    offs_in, rate_in, child, row_in, col_w, prio_in, par_ref, out_ref,
    offs, rate, row_w, prio_ref, xbuf, cbuf, whi, wlo, wide_w, acc,
    gt, snd, land, relay, slab, half, q, mrg, nat, part, prit, edge, halo, fin, parv, outv,
    ms, cs, ws, ps, os, zs, zr, fs, fr, ys, yr, hs, hr,
):
    n, me = lax.axis_index("nest"), lax.axis_index("tile")
    tiles, nests = lax.axis_size("tile"), lax.axis_size("nest")
    cols, rows = tiles * XB, tiles * CELL
    own = par_ref.shape[1]
    chunks, pieces, depth, piece = xbuf.shape
    crow = row_w.shape[1]
    chips, chip, core = tiles // 2, me // 2, lax.rem(me, 2)
    other = 2 * chip + 1 - core
    high = FC * CELL

    def child_copy(k, c):
        start = c * piece if isinstance(c, int) else pl.multiple_of(c * piece, 128)
        return pltpu.make_async_copy(
            child.at[pl.ds(k * depth, depth), pl.ds(start, piece)], xbuf.at[k, c], cs.at[k, c]
        )

    def weight_copy(c):
        start = c * piece if isinstance(c, int) else pl.multiple_of(c * piece, 128)
        return pltpu.make_async_copy(col_w.at[pl.ds(start, piece), :], cbuf.at[c], ws.at[c])

    small = [
        pltpu.make_async_copy(a, b, ms.at[i])
        for i, (a, b) in enumerate(((row_in, row_w), (offs_in, offs), (rate_in, rate), (prio_in, prio_ref)))
    ]
    small[0].start()
    for c in range(min(AHEAD, pieces)):
        child_copy(0, c).start()
        weight_copy(c).start()
    for c in small[1:]:
        c.start()

    barrier = pltpu.get_barrier_semaphore()
    peers = chips - 1 + nests - 1 + 2

    @pl.loop(1, chips)
    def _(j):
        d = 2 * lax.rem(chip + j, chips) + core
        pl.semaphore_signal(barrier, inc=1, device_id=(n, d), device_id_type=MESH)

    for dn in range(1, nests):
        pl.semaphore_signal(barrier, inc=1, device_id=(lax.rem(n + dn, nests), me), device_id_type=MESH)
    for dt in (1, tiles - 1):
        pl.semaphore_signal(barrier, inc=1, device_id=(n, lax.rem(me + dt, tiles)), device_id_type=MESH)

    def spread_row_weights():
        a = lax.broadcasted_iota(jnp.int32, (high, CELL), 0)
        b = lax.broadcasted_iota(jnp.int32, (high, CELL), 1)
        down = (a // FC == b).astype(f32).astype(bf16)
        a = lax.broadcasted_iota(jnp.int32, (crow, depth), 0)
        b = lax.broadcasted_iota(jnp.int32, (crow, depth), 1)
        across = (lax.rem(b, crow) == a).astype(f32).astype(bf16)
        a = lax.broadcasted_iota(jnp.int32, (high, depth), 0)
        b = lax.broadcasted_iota(jnp.int32, (high, depth), 1)
        same = lax.rem(a, FC) == b // crow
        for i, w in enumerate(two_parts(row_w[...])):
            full = mm(mm(down, w).astype(bf16), across)
            wide_w[i * high : (i + 1) * high, :] = jnp.where(same, full, 0.0).astype(bf16)

    step = min(256, piece)
    block = min(256, cols)

    def compute(k):
        acc[k] = jnp.zeros(acc.shape[1:], f32)

        @pl.loop(0, pieces)
        def _(c):
            child_copy(k, c).wait()
            if k == 0:
                weight_copy(c).wait()

                @pl.when(c + AHEAD < pieces)
                def _():
                    child_copy(0, c + AHEAD).start()
                    weight_copy(c + AHEAD).start()

            if k + 1 < chunks:
                child_copy(k + 1, c).start()
            left_high, left_low = [], []
            for s in range(piece // step):
                xh, xl = two_parts(xbuf[k, c, :, s * step : (s + 1) * step])
                t = mm(wide_w[...], xh)
                t = t[:high] + t[high:] + mm(wide_w[0:high, :], xl)
                th, tl = two_parts(t)
                left_high.append(th)
                left_low.append(tl)
            a_high = jnp.concatenate(left_high, 1)
            a = jnp.concatenate([a_high, jnp.concatenate(left_low, 1)], 0)
            for b in range(cols // block):
                span = pl.ds(b * block, block)
                if k == 0:
                    wh, wl = two_parts(cbuf[c, :, span])
                    whi[c, :, span] = wh
                    wlo[c, :, span] = wl
                else:
                    wh, wl = whi[c, :, span], wlo[c, :, span]
                u = mm(a, wh)
                acc[k, :, span] += u[:high] + u[high:] + mm(a_high, wl)

    def turn(k):
        wide = min(128, cols)
        for b in range(cols // wide):
            gt[k, b * wide : (b + 1) * wide, :] = acc[k, :, b * wide : (b + 1) * wide].T
        gt[k, cols : cols + 8, :] = gt[k, 0:8, :]

    def send_tiles(k, h):
        left = offs[1, n]

        @pl.loop(0, chips, step=4)
        def _(j0):
            for dj in range(4):
                for c in range(2):
                    s = lax.rem(2 * XB * (j0 + dj) + XB * c + 8 * h - left + cols, cols)
                    snd[k, h, j0 + dj, c] = swap_rows_and_groups(gt[k, pl.ds(s, 8), :])

        @pl.loop(0, chips - 1)
        def _(i):
            j = lax.select(lax.rem(i, 2) == 0, i // 2 + 1, chips - 1 - i // 2)
            d = lax.rem(chip + j, chips)
            pltpu.make_async_remote_copy(
                src_ref=snd.at[k, h, d],
                dst_ref=land.at[k, h, chip],
                send_sem=zs.at[k, h],
                recv_sem=zr.at[k, h],
                device_id=(n, 2 * d + core),
                device_id_type=MESH,
            ).start()

        land[k, h, chip] = snd[k, h, chip]

    def pass_on(k, h):
        got = land.at[k, h, pl.ds(0, chips - 1)]
        pltpu.make_async_copy(got, got, zr.at[k, h]).wait()
        copy = pltpu.make_async_remote_copy(
            src_ref=land.at[k, h, :, 1 - core],
            dst_ref=relay.at[k, h],
            send_sem=fs.at[k, h],
            recv_sem=fr.at[k, h],
            device_id=(n, other),
            device_id_type=MESH,
        )
        copy.start()
        passed[k, h] = copy

    def send_nests(k, h):
        passed[k, h].wait()
        top = offs[0, n]

        @pl.loop(0, chips, step=4)
        def _(i0):
            for di in range(4):
                i = i0 + di
                slab[pl.ds(pl.multiple_of(16 * i + 8 * core, 8), 8), :] = land[k, h, i, core]
                slab[pl.ds(pl.multiple_of(16 * i + 8 - 8 * core, 8), 8), :] = relay[k, h, i]

        slab[rows : rows + 8, :] = slab[0:8, :]

        @pl.loop(0, rows // 8, step=8)
        def _(g0):
            for dg in range(8):
                g = g0 + dg
                s = lax.rem(8 * g - top + rows, rows)
                half[k, h, pl.ds(pl.multiple_of(8 * g, 8), 8), :] = slab[pl.ds(s, 8), :]

        for dn in (2, 1, 3):
            b = lax.rem(n + dn, nests)
            start = pl.multiple_of(lax.rem(b * own, rows), own)
            pltpu.make_async_remote_copy(
                src_ref=half.at[k, h, pl.ds(start, own), :],
                dst_ref=q.at[k, h, n],
                send_sem=ys.at[k, h],
                recv_sem=yr.at[k, h],
                device_id=(b, me),
                device_id_type=MESH,
            ).start()
        mine = pl.multiple_of(lax.rem(n * own, rows), own)

        @pl.loop(0, own // 8)
        def _(g):
            r = pl.multiple_of(8 * g, 8)
            q[k, h, n, pl.ds(r, 8), :] = half[k, h, pl.ds(mine + r, 8), :]

    span = min(128, own)
    taken = [
        pltpu.make_async_copy(par_ref.at[:, pl.ds(b * span, span)], parv.at[b], ps.at[b]) for b in range(own // span)
    ]

    def to_rows(dst):
        for lb in range(TILED):
            for yb in range(own // span):
                dst[lb, yb * span : (yb + 1) * span, :] = nat[
                    lb * 128 : (lb + 1) * 128, yb * span : (yb + 1) * span
                ].T

    def own_rows():
        small[3].wait()
        for x in range(XB):
            nat[x * FC : (x + 1) * FC, :] = jnp.broadcast_to(prio_ref[x : x + 1, :].astype(f32), (FC, own))
        to_rows(prit)
        for c in taken:
            c.wait()
        for k in range(chunks):
            for x in range(XB):
                for b in range(own // span):
                    nat[x * FC : (x + 1) * FC, b * span : (b + 1) * span] = parv[
                        b, pl.ds(k * XB * FC + x, FC, stride=XB), :
                    ]
            to_rows(part.at[k])

    packs = min(8, own // 8)
    packed = own // packs
    lane = lax.broadcasted_iota(jnp.int32, (8, 128), 1)
    east, west = lax.rem(me + 1, tiles), lax.rem(me + tiles - 1, tiles)
    up, down = lax.rem(n + 1, nests), lax.rem(n + nests - 1, nests)
    flights, passed, given = {}, {}, []

    def merge(k, h):
        got = q.at[k, h, pl.ds(0, nests - 1)]
        pltpu.make_async_copy(got, got, yr.at[k, h]).wait()

        @pl.loop(0, own // 8, step=4)
        def _(g0):
            for dg in range(4):
                r = pl.ds(pl.multiple_of(8 * (g0 + dg), 8), 8)
                v, p = part[k, h, r, :], prit[h, r, :]
                for m in range(nests):
                    v = jnp.where(p == float(m), q[k, h, m, r, :], v)
                mrg[k, h, pl.ds(pl.multiple_of(8 * (g0 + dg) + 8, 8), 8), :] = v

        moves = [
            (mrg.at[k, h, pl.ds(8, 8), :], mrg.at[k, h, pl.ds(own + 8, 8), :], (down, me)),
            (mrg.at[k, h, pl.ds(own, 8), :], mrg.at[k, h, pl.ds(0, 8), :], (up, me)),
        ]
        for side, tile, to in ((0, 0, west), (1, TILED - 1, east)):
            if h != tile:
                continue
            for i in range(packed // 8):
                e = jnp.zeros((8, 128), f32)
                for j in range(packs):
                    a = mrg[k, h, 8 + packed * j + 8 * i : 16 + packed * j + 8 * i, :]
                    shift = (FC * (j + side)) % 128
                    e = jnp.where(lane // FC == j, pltpu.roll(a, shift, 1) if shift else a, e)
                edge[k, side, 8 * i : 8 * i + 8, :] = e
            moves.append((edge.at[k, side], halo.at[k, side], (n, to)))
        copies = [
            pltpu.make_async_remote_copy(
                src_ref=s, dst_ref=d, send_sem=hs.at[k, h, i], recv_sem=hr.at[k, h, i], device_id=to, device_id_type=MESH
            )
            for i, (s, d, to) in enumerate(moves)
        ]
        for c in copies:
            c.start()
        flights.setdefault(k, []).extend(copies)

    def finish(k):
        for c in flights[k]:
            c.wait()
        mrg[k, :, 7:8, :] = jnp.where(n == 0, mrg[k, :, 8:9, :], mrg[k, :, 7:8, :])
        mrg[k, :, own + 8 : own + 9, :] = jnp.where(
            n == nests - 1, mrg[k, :, own + 7 : own + 8, :], mrg[k, :, own + 8 : own + 9, :]
        )
        r = jnp.zeros((8, 128), f32)
        for f in range(FC):
            r = jnp.where(lax.rem(lane, FC) == f, rate[k * FC + f], r)

        for j in range(packs):
            @pl.loop(0, packed // 8)
            def _(i):
                o = pl.multiple_of(packed * j + 8 * i, 8)
                e = halo[k, 0, pl.ds(pl.multiple_of(8 * i, 8), 8), :]
                w = halo[k, 1, pl.ds(pl.multiple_of(8 * i, 8), 8), :]
                es, ws_ = (128 - FC - FC * j) % 128, (128 - FC * j) % 128
                e = pltpu.roll(e, es, 1) if es else e
                w = pltpu.roll(w, ws_, 1) if ws_ else w
                mid = [mrg[k, t, pl.ds(o + 8, 8), :] for t in range(TILED)]
                east_of = [pltpu.roll(c, 128 - FC, 1) for c in mid] + [e]
                west_of = [w] + [pltpu.roll(c, FC, 1) for c in mid]
                for t in range(TILED):
                    c = mid[t]
                    north, south = mrg[k, t, pl.ds(o + 9, 8), :], mrg[k, t, pl.ds(o + 7, 8), :]
                    east_side = jnp.where(lane >= 128 - FC, east_of[t + 1], east_of[t])
                    west_side = jnp.where(lane < FC, west_of[t], west_of[t + 1])
                    fin[t, pl.ds(o, 8), :] = c + r * (east_side + west_side + north + south - 4.0 * c)

        for lb in range(TILED):
            for yb in range(own // span):
                t = fin[lb, yb * span : (yb + 1) * span, :].T
                for x in range(8):
                    outv[yb, pl.ds(k * XB * FC + lb * 8 + x, FC, stride=XB), :] = t[x * FC : (x + 1) * FC, :]
        r = pl.ds(k * XB * FC, XB * FC)
        for b in range(own // span):
            c = pltpu.make_async_copy(outv.at[b, r, :], out_ref.at[r, pl.ds(b * span, span)], os.at[k, b])
            c.start()
            given.append(c)

    small[0].wait()
    spread_row_weights()
    for k in range(chunks):
        compute(k)
        if k == 0:
            for c in taken:
                c.start()
            for c in small[1:3]:
                c.wait()
        turn(k)
        if k == 0:
            pl.semaphore_wait(barrier, peers)
        for h in range(TILED):
            send_tiles(k, h)
    own_rows()
    order = [(k, h) for k in range(chunks) for h in range(TILED)]
    for i, (k, h) in enumerate(order):
        pass_on(k, h)
        if i >= 2:
            merge(*order[i - 2])
        send_nests(k, h)
    for i, (k, h) in enumerate(order[-2:]):
        if i == 0:
            for done in range(chunks - 1):
                finish(done)
        merge(k, h)
    finish(chunks - 1)
    for c in given:
        c.wait()
    for k, h in order:
        sent = land.at[k, h, pl.ds(0, chips - 1)]
        pltpu.make_async_copy(sent, sent, zs.at[k, h]).wait()
        sent = q.at[k, h, pl.ds(0, nests - 1)]
        pltpu.make_async_copy(sent, sent, ys.at[k, h]).wait()


def feedback(offs, rate, child, row_w, col_w, prio, par, tiles, nests):
    own = par.shape[1]
    chunks = par.shape[0] // XB // FC
    cols, rows = tiles * XB, tiles * CELL
    span = min(128, own)
    depth = FC * row_w.shape[1]
    width = child.shape[1]
    pieces = min(6, width // 128)
    piece = width // pieces
    packed = own // min(8, own // 8)
    hbm = pl.BlockSpec(memory_space=pltpu.HBM)
    dma = pltpu.SemaphoreType.DMA
    return pl.pallas_call(
        kernel,
        out_shape=jax.ShapeDtypeStruct(par.shape, f32),
        in_specs=[hbm] * 7,
        out_specs=pl.BlockSpec(memory_space=pl.ANY),
        scratch_shapes=[
            pltpu.SMEM(offs.shape, jnp.int32),
            pltpu.SMEM(rate.shape, f32),
            pltpu.VMEM(row_w.shape, f32),
            pltpu.VMEM(prio.shape, jnp.int32),
            pltpu.VMEM((chunks, pieces, depth, piece), f32),
            pltpu.VMEM((pieces, piece, cols), f32),
            pltpu.VMEM((pieces, piece, cols), bf16),
            pltpu.VMEM((pieces, piece, cols), bf16),
            pltpu.VMEM((2 * FC * CELL, depth), bf16),
            pltpu.VMEM((chunks, FC * CELL, cols), f32),
            pltpu.VMEM((chunks, cols + 8, 128), f32),
            pltpu.VMEM((chunks, TILED, tiles // 2, 2, CELL, 128), f32),
            pltpu.VMEM((chunks, TILED, tiles // 2, 2, CELL, 128), f32),
            pltpu.VMEM((chunks, TILED, tiles // 2, CELL, 128), f32),
            pltpu.VMEM((rows + 8, 128), f32),
            pltpu.VMEM((chunks, TILED, rows, 128), f32),
            pltpu.VMEM((chunks, TILED, nests, own, 128), f32),
            pltpu.VMEM((chunks, TILED, own + 16, 128), f32),
            pltpu.VMEM((XB * FC, own), f32),
            pltpu.VMEM((chunks, TILED, own, 128), f32),
            pltpu.VMEM((TILED, own, 128), f32),
            pltpu.VMEM((chunks, 2, packed, 128), f32),
            pltpu.VMEM((chunks, 2, packed, 128), f32),
            pltpu.VMEM((TILED, own, 128), f32),
            pltpu.VMEM((own // span, par.shape[0], span), f32),
            pltpu.VMEM((own // span, par.shape[0], span), f32),
            dma((4,)), dma((chunks, pieces)), dma((pieces,)), dma((own // span,)), dma((chunks, own // span)),
            dma((chunks, TILED)), dma((chunks, TILED)), dma((chunks, TILED)), dma((chunks, TILED)),
            dma((chunks, TILED)), dma((chunks, TILED)),
            dma((chunks, TILED, 4)), dma((chunks, TILED, 4)),
        ],
        compiler_params=pltpu.CompilerParams(
            collective_id=0, has_side_effects=True, vmem_limit_bytes=52 * 1024 * 1024
        ),
    )(offs, rate, child, row_w, col_w, prio, par)


def per_device(child_fields, row_weights, col_weights, nest_offsets, priority, parent_old, smooth_rate):
    fields, strip, own = parent_old.shape
    tiles, nests = lax.axis_size("tile"), lax.axis_size("nest")
    child = child_fields.reshape(-1, child_fields.shape[3])
    par = parent_old.reshape(fields * strip, own)
    args = (nest_offsets.T, smooth_rate, child, row_weights, col_weights, priority, par)
    args = [pltpu.with_memory_space_constraint(a, pltpu.HBM) for a in args]
    out = feedback(*args, tiles, nests)
    return out.reshape(fields, strip, own)


def solution(mesh):
    return jax.shard_map(
        per_device,
        mesh=mesh,
        in_specs=(
            P("nest", None, "tile", None),
            P(),
            P(),
            P(),
            P("tile", "nest"),
            P(None, "tile", "nest"),
            P(),
        ),
        out_specs=P(None, "tile", "nest"),
        check_vma=False,
    )
```

```python
import jax
import jax.numpy as jnp
from jax import lax
from jax.experimental import pallas as pl
from jax.experimental.pallas import tpu as pltpu
from jax.sharding import PartitionSpec as P

MESH = pl.DeviceIdType.MESH
CELL = 8
FC = 16
XB = 16
TILED = XB * FC // 128
AHEAD = 3
STRIDE = 13
f32, bf16 = jnp.float32, jnp.bfloat16


def swap_rows_and_groups(v):
    sub = lax.broadcasted_iota(jnp.int32, v.shape, 0)
    lane = lax.broadcasted_iota(jnp.int32, v.shape, 1)
    for d in (1, 2, 4):
        w = FC * d
        low = pltpu.roll(pltpu.roll(v, CELL - d, 0), w, 1)
        high = low if 2 * d == CELL else pltpu.roll(pltpu.roll(v, d, 0), 128 - w, 1)
        sbit, lbit = (sub & d) != 0, (lane & w) != 0
        v = jnp.where(sbit == lbit, v, jnp.where(lbit, low, high))
    return v


def two_parts(v):
    high = v.astype(bf16)
    return high, (v - high.astype(f32)).astype(bf16)


def mm(a, b):
    return jnp.dot(a, b, preferred_element_type=f32)


def kernel(
    offs_in, rate_in, child, row_in, col_w, prio_in, par_ref, out_ref,
    offs, rate, row_w, prio_ref, xbuf, cbuf, whi, wlo, wide_w, acc,
    gt, snd, land, relay, slab, half, q, mrg, nat, part, prit, edge, halo, fin, parv, outv,
    ms, cs, ws, ps, os, zs, zr, fs, fr, ys, yr, hs, hr,
):
    n, me = lax.axis_index("nest"), lax.axis_index("tile")
    tiles, nests = lax.axis_size("tile"), lax.axis_size("nest")
    cols, rows = tiles * XB, tiles * CELL
    own = par_ref.shape[1]
    chunks, pieces, depth, piece = xbuf.shape
    crow = row_w.shape[1]
    chips, chip, core = tiles // 2, me // 2, lax.rem(me, 2)
    other = 2 * chip + 1 - core
    high = FC * CELL

    def child_copy(k, c):
        start = c * piece if isinstance(c, int) else pl.multiple_of(c * piece, 128)
        return pltpu.make_async_copy(
            child.at[pl.ds(k * depth, depth), pl.ds(start, piece)], xbuf.at[k, c], cs.at[k, c]
        )

    def weight_copy(c):
        start = c * piece if isinstance(c, int) else pl.multiple_of(c * piece, 128)
        return pltpu.make_async_copy(col_w.at[pl.ds(start, piece), :], cbuf.at[c], ws.at[c])

    small = [
        pltpu.make_async_copy(a, b, ms.at[i])
        for i, (a, b) in enumerate(((row_in, row_w), (offs_in, offs), (rate_in, rate), (prio_in, prio_ref)))
    ]
    small[0].start()
    ahead = next(a for a in range(min(AHEAD, pieces), 0, -1) if pieces % a == 0)
    for c in range(ahead):
        child_copy(0, c).start()
        weight_copy(c).start()
    for c in small[1:]:
        c.start()

    barrier = pltpu.get_barrier_semaphore()
    peers = chips - 1 + nests - 1 + 2

    @pl.loop(1, chips)
    def _(j):
        d = 2 * lax.rem(chip + j, chips) + core
        pl.semaphore_signal(barrier, inc=1, device_id=(n, d), device_id_type=MESH)

    for dn in range(1, nests):
        pl.semaphore_signal(barrier, inc=1, device_id=(lax.rem(n + dn, nests), me), device_id_type=MESH)
    for dt in (1, tiles - 1):
        pl.semaphore_signal(barrier, inc=1, device_id=(n, lax.rem(me + dt, tiles)), device_id_type=MESH)

    def spread_row_weights():
        a = lax.broadcasted_iota(jnp.int32, (high, CELL), 0)
        b = lax.broadcasted_iota(jnp.int32, (high, CELL), 1)
        down = (a // FC == b).astype(f32).astype(bf16)
        a = lax.broadcasted_iota(jnp.int32, (crow, depth), 0)
        b = lax.broadcasted_iota(jnp.int32, (crow, depth), 1)
        across = (lax.rem(b, crow) == a).astype(f32).astype(bf16)
        a = lax.broadcasted_iota(jnp.int32, (high, depth), 0)
        b = lax.broadcasted_iota(jnp.int32, (high, depth), 1)
        same = lax.rem(a, FC) == b // crow
        for i, w in enumerate(two_parts(row_w[...])):
            full = mm(mm(down, w).astype(bf16), across)
            wide_w[i * high : (i + 1) * high, :] = jnp.where(same, full, 0.0).astype(bf16)

    step = min(256, piece)
    block = min(256, cols)

    def compute(k):
        acc[k] = jnp.zeros(acc.shape[1:], f32)

        @pl.loop(0, pieces)
        def _(c):
            child_copy(k, c).wait()
            if k == 0:
                weight_copy(c).wait()

                @pl.when(c + ahead < pieces)
                def _():
                    child_copy(0, c + ahead).start()
                    weight_copy(c + ahead).start()

                for later in range(1, chunks):
                    @pl.when(c + ahead >= pieces)
                    def _():
                        for i in range(pieces // ahead):
                            child_copy(later, (c + ahead - pieces) * (pieces // ahead) + i).start()
            left_high, left_low = [], []
            for s in range(piece // step):
                xh, xl = two_parts(xbuf[k, c, :, s * step : (s + 1) * step])
                t = mm(wide_w[...], xh)
                t = t[:high] + t[high:] + mm(wide_w[0:high, :], xl)
                th, tl = two_parts(t)
                left_high.append(th)
                left_low.append(tl)
            a_high = jnp.concatenate(left_high, 1)
            a = jnp.concatenate([a_high, jnp.concatenate(left_low, 1)], 0)
            for b in range(cols // block):
                span = pl.ds(b * block, block)
                if k == 0:
                    wh, wl = two_parts(cbuf[c, :, span])
                    whi[c, :, span] = wh
                    wlo[c, :, span] = wl
                else:
                    wh, wl = whi[c, :, span], wlo[c, :, span]
                u = mm(a, wh)
                acc[k, :, span] += u[:high] + u[high:] + mm(a_high, wl)

    def turn(k):
        wide = min(128, cols)
        for b in range(cols // wide):
            gt[k, b * wide : (b + 1) * wide, :] = acc[k, :, b * wide : (b + 1) * wide].T
        gt[k, cols : cols + 8, :] = gt[k, 0:8, :]

    def send_tiles(k, h):
        left = offs[1, n]

        batch = min(16, chips)

        @pl.loop(0, chips, step=batch)
        def _(j0):
            for dj in range(batch):
                for c in range(2):
                    s = lax.rem(2 * XB * (j0 + dj) + XB * c + 8 * h - left + cols, cols)
                    snd[k, h, j0 + dj, c] = swap_rows_and_groups(gt[k, pl.ds(s, 8), :])

        for i in range(chips - 1):
            d = lax.rem(chip + (i + 1) * STRIDE % chips, chips)
            pltpu.make_async_remote_copy(
                src_ref=snd.at[k, h, d],
                dst_ref=land.at[k, h, chip],
                send_sem=zs.at[k, h],
                recv_sem=zr.at[k, h],
                device_id=(n, 2 * d + core),
                device_id_type=MESH,
            ).start()

        land[k, h, chip] = snd[k, h, chip]

    def pass_on(k, h):
        got = land.at[k, h, pl.ds(0, chips - 1)]
        pltpu.make_async_copy(got, got, zr.at[k, h]).wait()
        copy = pltpu.make_async_remote_copy(
            src_ref=land.at[k, h, :, 1 - core],
            dst_ref=relay.at[k, h],
            send_sem=fs.at[k, h],
            recv_sem=fr.at[k, h],
            device_id=(n, other),
            device_id_type=MESH,
        )
        copy.start()
        passed[k, h] = copy

    def send_nests(k, h):
        passed[k, h].wait()
        top = offs[0, n]

        @pl.loop(0, chips, step=4)
        def _(i0):
            for di in range(4):
                i = i0 + di
                slab[pl.ds(pl.multiple_of(16 * i + 8 * core, 8), 8), :] = land[k, h, i, core]
                slab[pl.ds(pl.multiple_of(16 * i + 8 - 8 * core, 8), 8), :] = relay[k, h, i]

        slab[rows : rows + 8, :] = slab[0:8, :]

        @pl.loop(0, rows // 8, step=8)
        def _(g0):
            for dg in range(8):
                g = g0 + dg
                s = lax.rem(8 * g - top + rows, rows)
                half[k, h, pl.ds(pl.multiple_of(8 * g, 8), 8), :] = slab[pl.ds(s, 8), :]

        for dn in (2, 1, 3):
            b = lax.rem(n + dn, nests)
            start = pl.multiple_of(lax.rem(b * own, rows), own)
            pltpu.make_async_remote_copy(
                src_ref=half.at[k, h, pl.ds(start, own), :],
                dst_ref=q.at[k, h, n],
                send_sem=ys.at[k, h],
                recv_sem=yr.at[k, h],
                device_id=(b, me),
                device_id_type=MESH,
            ).start()
        mine = pl.multiple_of(lax.rem(n * own, rows), own)

        q[k, h, n] = half[k, h, pl.ds(mine, own), :]

    span = min(128, own)
    taken = [
        pltpu.make_async_copy(par_ref.at[:, pl.ds(b * span, span)], parv.at[b], ps.at[b]) for b in range(own // span)
    ]

    def to_rows(dst):
        for lb in range(TILED):
            for yb in range(own // span):
                dst[lb, yb * span : (yb + 1) * span, :] = nat[
                    lb * 128 : (lb + 1) * 128, yb * span : (yb + 1) * span
                ].T

    def own_rows():
        small[3].wait()
        for x in range(XB):
            nat[x * FC : (x + 1) * FC, :] = jnp.broadcast_to(prio_ref[x : x + 1, :].astype(f32), (FC, own))
        to_rows(prit)
        for c in taken:
            c.wait()
        for k in range(chunks):
            for x in range(XB):
                for b in range(own // span):
                    nat[x * FC : (x + 1) * FC, b * span : (b + 1) * span] = parv[
                        b, pl.ds(k * XB * FC + x, FC, stride=XB), :
                    ]
            to_rows(part.at[k])

    packs = min(8, own // 8)
    packed = own // packs
    lane = lax.broadcasted_iota(jnp.int32, (8, 128), 1)
    east, west = lax.rem(me + 1, tiles), lax.rem(me + tiles - 1, tiles)
    up, down = lax.rem(n + 1, nests), lax.rem(n + nests - 1, nests)
    flights, passed, given = {}, {}, []

    def merge(k, h):
        got = q.at[k, h, pl.ds(0, nests - 1)]
        pltpu.make_async_copy(got, got, yr.at[k, h]).wait()

        for g in range(own // 8):
            r = slice(8 * g, 8 * g + 8)
            v, p = part[k, h, r, :], prit[h, r, :]
            for m in range(nests):
                v = jnp.where(p == float(m), q[k, h, m, r, :], v)
            mrg[k, h, 8 * g + 8 : 8 * g + 16, :] = v

        moves = [
            (mrg.at[k, h, pl.ds(8, 8), :], mrg.at[k, h, pl.ds(own + 8, 8), :], (down, me)),
            (mrg.at[k, h, pl.ds(own, 8), :], mrg.at[k, h, pl.ds(0, 8), :], (up, me)),
        ]
        for side, tile, to in ((0, 0, west), (1, TILED - 1, east)):
            if h != tile:
                continue
            for i in range(packed // 8):
                e = jnp.zeros((8, 128), f32)
                for j in range(packs):
                    a = mrg[k, h, 8 + packed * j + 8 * i : 16 + packed * j + 8 * i, :]
                    shift = (FC * (j + side)) % 128
                    e = jnp.where(lane // FC == j, pltpu.roll(a, shift, 1) if shift else a, e)
                edge[k, side, 8 * i : 8 * i + 8, :] = e
            moves.append((edge.at[k, side], halo.at[k, side], (n, to)))
        copies = [
            pltpu.make_async_remote_copy(
                src_ref=s, dst_ref=d, send_sem=hs.at[k, h, i], recv_sem=hr.at[k, h, i], device_id=to, device_id_type=MESH
            )
            for i, (s, d, to) in enumerate(moves)
        ]
        for c in copies:
            c.start()
        flights.setdefault(k, []).extend(copies)

    def finish(k):
        for c in flights[k]:
            c.wait()
        mrg[k, :, 7:8, :] = jnp.where(n == 0, mrg[k, :, 8:9, :], mrg[k, :, 7:8, :])
        mrg[k, :, own + 8 : own + 9, :] = jnp.where(
            n == nests - 1, mrg[k, :, own + 7 : own + 8, :], mrg[k, :, own + 8 : own + 9, :]
        )
        r = jnp.zeros((8, 128), f32)
        for f in range(FC):
            r = jnp.where(lax.rem(lane, FC) == f, rate[k * FC + f], r)

        for j in range(packs):
            for i in range(packed // 8):
                o = packed * j + 8 * i
                e = halo[k, 0, 8 * i : 8 * i + 8, :]
                w = halo[k, 1, 8 * i : 8 * i + 8, :]
                es, ws_ = (128 - FC - FC * j) % 128, (128 - FC * j) % 128
                e = pltpu.roll(e, es, 1) if es else e
                w = pltpu.roll(w, ws_, 1) if ws_ else w
                mid = [mrg[k, t, pl.ds(o + 8, 8), :] for t in range(TILED)]
                east_of = [pltpu.roll(c, 128 - FC, 1) for c in mid] + [e]
                west_of = [w] + [pltpu.roll(c, FC, 1) for c in mid]
                for t in range(TILED):
                    c = mid[t]
                    north, south = mrg[k, t, pl.ds(o + 9, 8), :], mrg[k, t, pl.ds(o + 7, 8), :]
                    east_side = jnp.where(lane >= 128 - FC, east_of[t + 1], east_of[t])
                    west_side = jnp.where(lane < FC, west_of[t], west_of[t + 1])
                    fin[t, pl.ds(o, 8), :] = c + r * (east_side + west_side + north + south - 4.0 * c)

        for lb in range(TILED):
            for yb in range(own // span):
                t = fin[lb, yb * span : (yb + 1) * span, :].T
                for x in range(8):
                    outv[yb, pl.ds(k * XB * FC + lb * 8 + x, FC, stride=XB), :] = t[x * FC : (x + 1) * FC, :]
        r = pl.ds(k * XB * FC, XB * FC)
        for b in range(own // span):
            c = pltpu.make_async_copy(outv.at[b, r, :], out_ref.at[r, pl.ds(b * span, span)], os.at[k, b])
            c.start()
            given.append(c)

    small[0].wait()
    spread_row_weights()
    for k in range(chunks):
        compute(k)
        if k == 0:
            for c in taken:
                c.start()
            for c in small[1:3]:
                c.wait()
        turn(k)
        if k == 0:
            pl.semaphore_wait(barrier, peers)
        if k:
            pass_on(k - 1, 0)
        for h in range(TILED):
            send_tiles(k, h)
            if k and h == 0:
                send_nests(k - 1, 0)
    own_rows()
    order = [(k, h) for k in range(chunks) for h in range(TILED)]
    waiting = []
    for k, h in order:
        if (k, h) not in passed:
            pass_on(k, h)
        if len(waiting) > 1:
            merge(*waiting.pop(0))
        if h or k == chunks - 1:
            send_nests(k, h)
        waiting.append((k, h))
    for i, (k, h) in enumerate(order[-2:]):
        if i == 0:
            for done in range(chunks - 1):
                finish(done)
        merge(k, h)
    finish(chunks - 1)
    for c in given:
        c.wait()
    for k, h in order:
        sent = land.at[k, h, pl.ds(0, chips - 1)]
        pltpu.make_async_copy(sent, sent, zs.at[k, h]).wait()
        sent = q.at[k, h, pl.ds(0, nests - 1)]
        pltpu.make_async_copy(sent, sent, ys.at[k, h]).wait()


def feedback(offs, rate, child, row_w, col_w, prio, par, tiles, nests):
    own = par.shape[1]
    chunks = par.shape[0] // XB // FC
    cols, rows = tiles * XB, tiles * CELL
    span = min(128, own)
    depth = FC * row_w.shape[1]
    width = child.shape[1]
    pieces = min(6, width // 128)
    piece = width // pieces
    packed = own // min(8, own // 8)
    hbm = pl.BlockSpec(memory_space=pltpu.HBM)
    dma = pltpu.SemaphoreType.DMA
    return pl.pallas_call(
        kernel,
        out_shape=jax.ShapeDtypeStruct(par.shape, f32),
        in_specs=[hbm] * 7,
        out_specs=pl.BlockSpec(memory_space=pl.ANY),
        scratch_shapes=[
            pltpu.SMEM(offs.shape, jnp.int32),
            pltpu.SMEM(rate.shape, f32),
            pltpu.VMEM(row_w.shape, f32),
            pltpu.VMEM(prio.shape, jnp.int32),
            pltpu.VMEM((chunks, pieces, depth, piece), f32),
            pltpu.VMEM((pieces, piece, cols), f32),
            pltpu.VMEM((pieces, piece, cols), bf16),
            pltpu.VMEM((pieces, piece, cols), bf16),
            pltpu.VMEM((2 * FC * CELL, depth), bf16),
            pltpu.VMEM((chunks, FC * CELL, cols), f32),
            pltpu.VMEM((chunks, cols + 8, 128), f32),
            pltpu.VMEM((chunks, TILED, tiles // 2, 2, CELL, 128), f32),
            pltpu.VMEM((chunks, TILED, tiles // 2, 2, CELL, 128), f32),
            pltpu.VMEM((chunks, TILED, tiles // 2, CELL, 128), f32),
            pltpu.VMEM((rows + 8, 128), f32),
            pltpu.VMEM((chunks, TILED, rows, 128), f32),
            pltpu.VMEM((chunks, TILED, nests, own, 128), f32),
            pltpu.VMEM((chunks, TILED, own + 16, 128), f32),
            pltpu.VMEM((XB * FC, own), f32),
            pltpu.VMEM((chunks, TILED, own, 128), f32),
            pltpu.VMEM((TILED, own, 128), f32),
            pltpu.VMEM((chunks, 2, packed, 128), f32),
            pltpu.VMEM((chunks, 2, packed, 128), f32),
            pltpu.VMEM((TILED, own, 128), f32),
            pltpu.VMEM((own // span, par.shape[0], span), f32),
            pltpu.VMEM((own // span, par.shape[0], span), f32),
            dma((4,)), dma((chunks, pieces)), dma((pieces,)), dma((own // span,)), dma((chunks, own // span)),
            dma((chunks, TILED)), dma((chunks, TILED)), dma((chunks, TILED)), dma((chunks, TILED)),
            dma((chunks, TILED)), dma((chunks, TILED)),
            dma((chunks, TILED, 4)), dma((chunks, TILED, 4)),
        ],
        compiler_params=pltpu.CompilerParams(
            collective_id=0, has_side_effects=True, vmem_limit_bytes=52 * 1024 * 1024
        ),
    )(offs, rate, child, row_w, col_w, prio, par)


def per_device(child_fields, row_weights, col_weights, nest_offsets, priority, parent_old, smooth_rate):
    fields, strip, own = parent_old.shape
    tiles, nests = lax.axis_size("tile"), lax.axis_size("nest")
    child = child_fields.reshape(-1, child_fields.shape[3])
    par = parent_old.reshape(fields * strip, own)
    args = (nest_offsets.T, smooth_rate, child, row_weights, col_weights, priority, par)
    args = [pltpu.with_memory_space_constraint(a, pltpu.HBM) for a in args]
    out = feedback(*args, tiles, nests)
    return out.reshape(fields, strip, own)


def solution(mesh):
    return jax.shard_map(
        per_device,
        mesh=mesh,
        in_specs=(
            P("nest", None, "tile", None),
            P(),
            P(),
            P(),
            P("tile", "nest"),
            P(None, "tile", "nest"),
            P(),
        ),
        out_specs=P(None, "tile", "nest"),
        check_vma=False,
    )
```

```python
import jax
import jax.numpy as jnp
from jax import lax
from jax.experimental import pallas as pl
from jax.experimental.pallas import tpu as pltpu
from jax.sharding import PartitionSpec as P

MESH = pl.DeviceIdType.MESH
CELL = 8
FC = 16
XB = 16
TILED = XB * FC // 128
AHEAD = 3
STRIDE = 13
f32, bf16 = jnp.float32, jnp.bfloat16


def swap_rows_and_groups(v):
    sub = lax.broadcasted_iota(jnp.int32, v.shape, 0)
    lane = lax.broadcasted_iota(jnp.int32, v.shape, 1)
    for d in (1, 2, 4):
        w = FC * d
        low = pltpu.roll(pltpu.roll(v, CELL - d, 0), w, 1)
        high = low if 2 * d == CELL else pltpu.roll(pltpu.roll(v, d, 0), 128 - w, 1)
        sbit, lbit = (sub & d) != 0, (lane & w) != 0
        v = jnp.where(sbit == lbit, v, jnp.where(lbit, low, high))
    return v


def two_parts(v):
    high = v.astype(bf16)
    return high, (v - high.astype(f32)).astype(bf16)


def mm(a, b):
    return jnp.dot(a, b, preferred_element_type=f32)


def kernel(
    offs_in, rate_in, child, row_in, col_w, prio_in, par_ref, out_ref,
    offs, rate, row_w, prio_ref, xbuf, cbuf, whi, wlo, wide_w, acc,
    gt, snd, land, relay, slab, half, q, mrg, nat, part, prit, edge, halo, fin, parv, outv,
    ms, cs, ws, ps, os, zs, zr, fs, fr, ys, yr, hs, hr,
):
    n, me = lax.axis_index("nest"), lax.axis_index("tile")
    tiles, nests = lax.axis_size("tile"), lax.axis_size("nest")
    cols, rows = tiles * XB, tiles * CELL
    own = par_ref.shape[1]
    chunks, pieces, depth, piece = xbuf.shape
    crow = row_w.shape[1]
    chips, chip, core = tiles // 2, me // 2, lax.rem(me, 2)
    other = 2 * chip + 1 - core
    high = FC * CELL

    def child_copy(k, c):
        start = c * piece if isinstance(c, int) else pl.multiple_of(c * piece, 128)
        return pltpu.make_async_copy(
            child.at[pl.ds(k * depth, depth), pl.ds(start, piece)], xbuf.at[k, c], cs.at[k, c]
        )

    def weight_copy(c):
        start = c * piece if isinstance(c, int) else pl.multiple_of(c * piece, 128)
        return pltpu.make_async_copy(col_w.at[pl.ds(start, piece), :], cbuf.at[c], ws.at[c])

    small = [
        pltpu.make_async_copy(a, b, ms.at[i])
        for i, (a, b) in enumerate(((row_in, row_w), (offs_in, offs), (rate_in, rate), (prio_in, prio_ref)))
    ]
    small[0].start()
    ahead = next(a for a in range(min(AHEAD, pieces), 0, -1) if pieces % a == 0)
    for c in range(ahead):
        child_copy(0, c).start()
        weight_copy(c).start()
    for c in small[1:]:
        c.start()

    barrier = pltpu.get_barrier_semaphore()
    peers = chips - 1 + nests - 1 + 2

    for j in range(1, chips):
        d = 2 * lax.rem(chip + j, chips) + core
        pl.semaphore_signal(barrier, inc=1, device_id=(n, d), device_id_type=MESH)

    for dn in range(1, nests):
        pl.semaphore_signal(barrier, inc=1, device_id=(lax.rem(n + dn, nests), me), device_id_type=MESH)
    for dt in (1, tiles - 1):
        pl.semaphore_signal(barrier, inc=1, device_id=(n, lax.rem(me + dt, tiles)), device_id_type=MESH)

    def spread_row_weights():
        a = lax.broadcasted_iota(jnp.int32, (high, CELL), 0)
        b = lax.broadcasted_iota(jnp.int32, (high, CELL), 1)
        down = (a // FC == b).astype(f32).astype(bf16)
        a = lax.broadcasted_iota(jnp.int32, (crow, depth), 0)
        b = lax.broadcasted_iota(jnp.int32, (crow, depth), 1)
        across = (lax.rem(b, crow) == a).astype(f32).astype(bf16)
        a = lax.broadcasted_iota(jnp.int32, (high, depth), 0)
        b = lax.broadcasted_iota(jnp.int32, (high, depth), 1)
        same = lax.rem(a, FC) == b // crow
        for i, w in enumerate(two_parts(row_w[...])):
            full = mm(mm(down, w).astype(bf16), across)
            wide_w[i * high : (i + 1) * high, :] = jnp.where(same, full, 0.0).astype(bf16)

    step = min(256, piece)
    block = min(256, cols)

    def compute(k):
        acc[k] = jnp.zeros(acc.shape[1:], f32)

        @pl.loop(0, pieces)
        def _(c):
            child_copy(k, c).wait()
            if k == 0:
                weight_copy(c).wait()

                @pl.when(c + ahead < pieces)
                def _():
                    child_copy(0, c + ahead).start()
                    weight_copy(c + ahead).start()

                for later in range(1, chunks):
                    @pl.when(c + ahead >= pieces)
                    def _():
                        for i in range(pieces // ahead):
                            child_copy(later, (c + ahead - pieces) * (pieces // ahead) + i).start()
            left_high, left_low = [], []
            for s in range(piece // step):
                xh, xl = two_parts(xbuf[k, c, :, s * step : (s + 1) * step])
                t = mm(wide_w[...], xh)
                t = t[:high] + t[high:] + mm(wide_w[0:high, :], xl)
                th, tl = two_parts(t)
                left_high.append(th)
                left_low.append(tl)
            a_high = jnp.concatenate(left_high, 1)
            a = jnp.concatenate([a_high, jnp.concatenate(left_low, 1)], 0)
            for b in range(cols // block):
                span = pl.ds(b * block, block)
                if k == 0:
                    wh, wl = two_parts(cbuf[c, :, span])
                    whi[c, :, span] = wh
                    wlo[c, :, span] = wl
                else:
                    wh, wl = whi[c, :, span], wlo[c, :, span]
                u = mm(a, wh)
                acc[k, :, span] += u[:high] + u[high:] + mm(a_high, wl)

    def turn(k):
        wide = min(128, cols)
        for b in range(cols // wide):
            gt[k, b * wide : (b + 1) * wide, :] = acc[k, :, b * wide : (b + 1) * wide].T
        gt[k, cols : cols + 8, :] = gt[k, 0:8, :]

    def send_tiles(k, h):
        left = offs[1, n]

        batch = min(16, chips)

        @pl.loop(0, chips, step=batch)
        def _(j0):
            for dj in range(batch):
                for c in range(2):
                    s = lax.rem(2 * XB * (j0 + dj) + XB * c + 8 * h - left + cols, cols)
                    snd[k, h, j0 + dj, c] = swap_rows_and_groups(gt[k, pl.ds(s, 8), :])

        for i in range(chips - 1):
            d = lax.rem(chip + (i + 1) * STRIDE % chips, chips)
            pltpu.make_async_remote_copy(
                src_ref=snd.at[k, h, d],
                dst_ref=land.at[k, h, chip],
                send_sem=zs.at[k, h],
                recv_sem=zr.at[k, h],
                device_id=(n, 2 * d + core),
                device_id_type=MESH,
            ).start()

        land[k, h, chip] = snd[k, h, chip]

    def pass_on(k, h):
        got = land.at[k, h, pl.ds(0, chips - 1)]
        pltpu.make_async_copy(got, got, zr.at[k, h]).wait()
        copy = pltpu.make_async_remote_copy(
            src_ref=land.at[k, h, :, 1 - core],
            dst_ref=relay.at[k, h],
            send_sem=fs.at[k, h],
            recv_sem=fr.at[k, h],
            device_id=(n, other),
            device_id_type=MESH,
        )
        copy.start()
        passed[k, h] = copy

    def send_nests(k, h):
        top = offs[0, n]
        for i in range(chips):
            slab[pl.ds(pl.multiple_of(16 * i + 8 * core, 8), 8), :] = land[k, h, i, core]
        passed[k, h].wait()
        for i in range(chips):
            slab[pl.ds(pl.multiple_of(16 * i + 8 - 8 * core, 8), 8), :] = relay[k, h, i]

        slab[rows : rows + 8, :] = slab[0:8, :]

        batch = min(16, own // 8)

        def turn_rows(c0):
            @pl.loop(0, own // 8, step=batch)
            def _(g0):
                for dg in range(batch):
                    r = c0 + 8 * (g0 + dg)
                    s = lax.rem(r - top + rows, rows)
                    half[k, h, pl.ds(pl.multiple_of(r, 8), 8), :] = slab[pl.ds(s, 8), :]

        here = pl.multiple_of(lax.rem(n * own, rows), own)
        away = pl.multiple_of(lax.rem((n + 1) * own, rows), own)
        turn_rows(here)
        for dn in (2, 1, 3):
            if dn == 1:
                turn_rows(away)
            b = lax.rem(n + dn, nests)
            start = pl.multiple_of(lax.rem(b * own, rows), own)
            pltpu.make_async_remote_copy(
                src_ref=half.at[k, h, pl.ds(start, own), :],
                dst_ref=q.at[k, h, n],
                send_sem=ys.at[k, h],
                recv_sem=yr.at[k, h],
                device_id=(b, me),
                device_id_type=MESH,
            ).start()
        mine = pl.multiple_of(lax.rem(n * own, rows), own)

        q[k, h, n] = half[k, h, pl.ds(mine, own), :]

    span = min(128, own)
    taken = [
        pltpu.make_async_copy(par_ref.at[:, pl.ds(b * span, span)], parv.at[b], ps.at[b]) for b in range(own // span)
    ]

    def to_rows(dst):
        for lb in range(TILED):
            for yb in range(own // span):
                dst[lb, yb * span : (yb + 1) * span, :] = nat[
                    lb * 128 : (lb + 1) * 128, yb * span : (yb + 1) * span
                ].T

    def own_rows():
        small[3].wait()
        for x in range(XB):
            nat[x * FC : (x + 1) * FC, :] = jnp.broadcast_to(prio_ref[x : x + 1, :].astype(f32), (FC, own))
        to_rows(prit)
        for c in taken:
            c.wait()
        for k in range(chunks):
            for x in range(XB):
                for b in range(own // span):
                    nat[x * FC : (x + 1) * FC, b * span : (b + 1) * span] = parv[
                        b, pl.ds(k * XB * FC + x, FC, stride=XB), :
                    ]
            to_rows(part.at[k])

    packs = min(8, own // 8)
    packed = own // packs
    lane = lax.broadcasted_iota(jnp.int32, (8, 128), 1)
    east, west = lax.rem(me + 1, tiles), lax.rem(me + tiles - 1, tiles)
    up, down = lax.rem(n + 1, nests), lax.rem(n + nests - 1, nests)
    flights, passed, given = {}, {}, []

    def merge(k, h):
        got = q.at[k, h, pl.ds(0, nests - 1)]
        pltpu.make_async_copy(got, got, yr.at[k, h]).wait()

        for g in range(own // 8):
            r = slice(8 * g, 8 * g + 8)
            v, p = part[k, h, r, :], prit[h, r, :]
            for m in range(nests):
                v = jnp.where(p == float(m), q[k, h, m, r, :], v)
            mrg[k, h, 8 * g + 8 : 8 * g + 16, :] = v

        moves = [
            (mrg.at[k, h, pl.ds(8, 8), :], mrg.at[k, h, pl.ds(own + 8, 8), :], (down, me)),
            (mrg.at[k, h, pl.ds(own, 8), :], mrg.at[k, h, pl.ds(0, 8), :], (up, me)),
        ]
        for side, tile, to in ((0, 0, west), (1, TILED - 1, east)):
            if h != tile:
                continue
            for i in range(packed // 8):
                e = jnp.zeros((8, 128), f32)
                for j in range(packs):
                    a = mrg[k, h, 8 + packed * j + 8 * i : 16 + packed * j + 8 * i, :]
                    shift = (FC * (j + side)) % 128
                    e = jnp.where(lane // FC == j, pltpu.roll(a, shift, 1) if shift else a, e)
                edge[k, side, 8 * i : 8 * i + 8, :] = e
            moves.append((edge.at[k, side], halo.at[k, side], (n, to)))
        copies = [
            pltpu.make_async_remote_copy(
                src_ref=s, dst_ref=d, send_sem=hs.at[k, h, i], recv_sem=hr.at[k, h, i], device_id=to, device_id_type=MESH
            )
            for i, (s, d, to) in enumerate(moves)
        ]
        for c in copies:
            c.start()
        flights.setdefault(k, []).extend(copies)

    def finish(k):
        for c in flights[k]:
            c.wait()
        mrg[k, :, 7:8, :] = jnp.where(n == 0, mrg[k, :, 8:9, :], mrg[k, :, 7:8, :])
        mrg[k, :, own + 8 : own + 9, :] = jnp.where(
            n == nests - 1, mrg[k, :, own + 7 : own + 8, :], mrg[k, :, own + 8 : own + 9, :]
        )
        r = jnp.zeros((8, 128), f32)
        for f in range(FC):
            r = jnp.where(lax.rem(lane, FC) == f, rate[k * FC + f], r)

        for j in range(packs):
            for i in range(packed // 8):
                o = packed * j + 8 * i
                e = halo[k, 0, 8 * i : 8 * i + 8, :]
                w = halo[k, 1, 8 * i : 8 * i + 8, :]
                es, ws_ = (128 - FC - FC * j) % 128, (128 - FC * j) % 128
                e = pltpu.roll(e, es, 1) if es else e
                w = pltpu.roll(w, ws_, 1) if ws_ else w
                mid = [mrg[k, t, pl.ds(o + 8, 8), :] for t in range(TILED)]
                east_of = [pltpu.roll(c, 128 - FC, 1) for c in mid] + [e]
                west_of = [w] + [pltpu.roll(c, FC, 1) for c in mid]
                for t in range(TILED):
                    c = mid[t]
                    north, south = mrg[k, t, pl.ds(o + 9, 8), :], mrg[k, t, pl.ds(o + 7, 8), :]
                    east_side = jnp.where(lane >= 128 - FC, east_of[t + 1], east_of[t])
                    west_side = jnp.where(lane < FC, west_of[t], west_of[t + 1])
                    fin[t, pl.ds(o, 8), :] = c + r * (east_side + west_side + north + south - 4.0 * c)

        for lb in range(TILED):
            for yb in range(own // span):
                t = fin[lb, yb * span : (yb + 1) * span, :].T
                for x in range(8):
                    outv[yb, pl.ds(k * XB * FC + lb * 8 + x, FC, stride=XB), :] = t[x * FC : (x + 1) * FC, :]
        r = pl.ds(k * XB * FC, XB * FC)
        for b in range(own // span):
            c = pltpu.make_async_copy(outv.at[b, r, :], out_ref.at[r, pl.ds(b * span, span)], os.at[k, b])
            c.start()
            given.append(c)

    small[0].wait()
    spread_row_weights()
    for k in range(chunks):
        compute(k)
        if k == 0:
            for c in taken:
                c.start()
            for c in small[1:3]:
                c.wait()
        turn(k)
        if k == 0:
            pl.semaphore_wait(barrier, peers)
        if k:
            pass_on(k - 1, 0)
        for h in range(TILED):
            send_tiles(k, h)
            if k and h == 0:
                send_nests(k - 1, 0)
    own_rows()
    order = [(k, h) for k in range(chunks) for h in range(TILED)]
    waiting = []
    for k, h in order:
        if (k, h) not in passed:
            pass_on(k, h)
        if len(waiting) > 1:
            merge(*waiting.pop(0))
        if h or k == chunks - 1:
            send_nests(k, h)
        waiting.append((k, h))
    for i, (k, h) in enumerate(order[-2:]):
        if i == 0:
            for done in range(chunks - 1):
                finish(done)
        merge(k, h)
    finish(chunks - 1)
    for c in given:
        c.wait()
    for k, h in order:
        sent = land.at[k, h, pl.ds(0, chips - 1)]
        pltpu.make_async_copy(sent, sent, zs.at[k, h]).wait()
        sent = q.at[k, h, pl.ds(0, nests - 1)]
        pltpu.make_async_copy(sent, sent, ys.at[k, h]).wait()


def feedback(offs, rate, child, row_w, col_w, prio, par, tiles, nests):
    own = par.shape[1]
    chunks = par.shape[0] // XB // FC
    cols, rows = tiles * XB, tiles * CELL
    span = min(128, own)
    depth = FC * row_w.shape[1]
    width = child.shape[1]
    pieces = min(6, width // 128)
    piece = width // pieces
    packed = own // min(8, own // 8)
    hbm = pl.BlockSpec(memory_space=pltpu.HBM)
    dma = pltpu.SemaphoreType.DMA
    return pl.pallas_call(
        kernel,
        out_shape=jax.ShapeDtypeStruct(par.shape, f32),
        in_specs=[hbm] * 7,
        out_specs=pl.BlockSpec(memory_space=pl.ANY),
        scratch_shapes=[
            pltpu.SMEM(offs.shape, jnp.int32),
            pltpu.SMEM(rate.shape, f32),
            pltpu.VMEM(row_w.shape, f32),
            pltpu.VMEM(prio.shape, jnp.int32),
            pltpu.VMEM((chunks, pieces, depth, piece), f32),
            pltpu.VMEM((pieces, piece, cols), f32),
            pltpu.VMEM((pieces, piece, cols), bf16),
            pltpu.VMEM((pieces, piece, cols), bf16),
            pltpu.VMEM((2 * FC * CELL, depth), bf16),
            pltpu.VMEM((chunks, FC * CELL, cols), f32),
            pltpu.VMEM((chunks, cols + 8, 128), f32),
            pltpu.VMEM((chunks, TILED, tiles // 2, 2, CELL, 128), f32),
            pltpu.VMEM((chunks, TILED, tiles // 2, 2, CELL, 128), f32),
            pltpu.VMEM((chunks, TILED, tiles // 2, CELL, 128), f32),
            pltpu.VMEM((rows + 8, 128), f32),
            pltpu.VMEM((chunks, TILED, rows, 128), f32),
            pltpu.VMEM((chunks, TILED, nests, own, 128), f32),
            pltpu.VMEM((chunks, TILED, own + 16, 128), f32),
            pltpu.VMEM((XB * FC, own), f32),
            pltpu.VMEM((chunks, TILED, own, 128), f32),
            pltpu.VMEM((TILED, own, 128), f32),
            pltpu.VMEM((chunks, 2, packed, 128), f32),
            pltpu.VMEM((chunks, 2, packed, 128), f32),
            pltpu.VMEM((TILED, own, 128), f32),
            pltpu.VMEM((own // span, par.shape[0], span), f32),
            pltpu.VMEM((own // span, par.shape[0], span), f32),
            dma((4,)), dma((chunks, pieces)), dma((pieces,)), dma((own // span,)), dma((chunks, own // span)),
            dma((chunks, TILED)), dma((chunks, TILED)), dma((chunks, TILED)), dma((chunks, TILED)),
            dma((chunks, TILED)), dma((chunks, TILED)),
            dma((chunks, TILED, 4)), dma((chunks, TILED, 4)),
        ],
        compiler_params=pltpu.CompilerParams(
            collective_id=0, has_side_effects=True, vmem_limit_bytes=52 * 1024 * 1024
        ),
    )(offs, rate, child, row_w, col_w, prio, par)


def per_device(child_fields, row_weights, col_weights, nest_offsets, priority, parent_old, smooth_rate):
    fields, strip, own = parent_old.shape
    tiles, nests = lax.axis_size("tile"), lax.axis_size("nest")
    child = child_fields.reshape(-1, child_fields.shape[3])
    par = parent_old.reshape(fields * strip, own)
    args = (nest_offsets.T, smooth_rate, child, row_weights, col_weights, priority, par)
    args = [pltpu.with_memory_space_constraint(a, pltpu.HBM) for a in args]
    out = feedback(*args, tiles, nests)
    return out.reshape(fields, strip, own)


def solution(mesh):
    return jax.shard_map(
        per_device,
        mesh=mesh,
        in_specs=(
            P("nest", None, "tile", None),
            P(),
            P(),
            P(),
            P("tile", "nest"),
            P(None, "tile", "nest"),
            P(),
        ),
        out_specs=P(None, "tile", "nest"),
        check_vma=False,
    )
```
